32 devices in a mesh: fsdp: 4 (over y, x), rep: 8 (over z, core).
Axes of the slice: x: 2, y: 2, z: 4, core: 2. Of those that a mesh axis runs over, the one named last changes fastest.
Arguments:
- hidden_in: bfloat16 [8192, 2048], P(('fsdp', 'rep'))
- out_grad: bfloat16 [8192, 2048], P(('fsdp', 'rep')), may hold values from -6 to 6
- attn_saved: bfloat16 [8192, 256], P(('fsdp', 'rep')), may hold values from -6 to 6
- row_lse: float32 [8192, 2], P(('fsdp', 'rep')), may hold values from 2.5 to 6
- w_qkv: bfloat16 [2048, 512], P('fsdp'), may hold values from -0.125 to 0.125
- w_out_t: bfloat16 [2048, 256], P('fsdp'), may hold values from -0.125 to 0.125
- doc_lengths: int32 [32, 4], P(('fsdp', 'rep')), may hold values from 1 to 128, 256 in all within a row
- seq_start: int32 [32], P(('fsdp', 'rep')), may hold values from 0 to 2047
Outputs:
- input_grad: bfloat16 [8192, 2048], P(('fsdp', 'rep'))
- grad_update: float32 [2048, 768], P('fsdp')
- grad_norm: float32 [], replicated
The draws below stay inside these ranges and needn't reach their ends.
Inputs may be any that keep to these rules, and one draw needn't show every extreme that they name: `doc_lengths`: each row sums to 256; the longest document of each device has exactly 128 tokens.
All inputs are finite; a program needn't handle non-finite values.
Results may differ from the reference program's by a relative error of at most 0.014.
Values may be sent and summed in bfloat16 or wider, within the bound.
A program may use at most 64 MiB of HBM per device.

```python
import math
import jax
import jax.numpy as jnp
import numpy as np
from jax import lax

D = 2048
HEAD = 128
QH = 2
DOCS = 4
SEQ = 256
QW = 256
COLS = 768
TOKENS = 8192
N_FSDP = 4
N_REP = 8


def draw_hidden_in(key, part):
    base_key = jax.random.fold_in(key, 101)
    noise = jax.random.normal(jax.random.fold_in(base_key, 1), (TOKENS, D), jnp.float32)
    ramp = 0.4 * 3.0 ** (jnp.arange(D, dtype=jnp.float32) / (D - 1))
    return (noise * ramp[None, :]).astype(jnp.bfloat16)


def with_ends(drawn, stream_key, least, largest):
    longest = drawn.shape.index(max(drawn.shape))
    spots = []
    for shift in (0, 1):
        where = [jax.random.randint(jax.random.fold_in(stream_key, axis), (), 0, length) for axis, length in enumerate(drawn.shape)]
        where[longest] = (where[longest] + shift) % drawn.shape[longest]
        spots.append(tuple(where))
    return drawn.at[spots[0]].set(least).at[spots[1]].set(largest)


def steps_of(stream_key, extent, pieces, low, high):
    loudness, own = 1.0, jax.random.fold_in(stream_key, 6)
    for axis_at, parts in pieces:
        heights = jnp.exp(jax.random.uniform(jax.random.fold_in(own, axis_at), (parts,), jnp.float32, low / len(pieces), high / len(pieces)))
        loudness = loudness * jnp.repeat(heights, extent[axis_at] // parts).reshape([-1 if axis == axis_at else 1 for axis in range(len(extent))])
    return loudness


def length_profile(amount, total, reach, slope):
    loads = [(1 << 20) // math.isqrt(grade ** slope) + 1 for grade in range(2, amount + 1)]
    rest, counts = total - reach - (amount - 1), [1] * (amount - 1)
    while rest > 0:
        movable = [i for i in range(amount - 1) if counts[i] < reach]
        mass, budget = sum([loads[i] for i in movable]), rest
        for i in movable:
            more = min(reach - counts[i], max(1, budget * loads[i] // mass), rest)
            counts[i] = counts[i] + more
            rest = rest - more
    return np.array([reach] + counts)


def uneven_parts(rng, amount, total, bound, slope):
    if amount == 2:
        one = jax.random.randint(rng, (), max(1, total - bound), min(bound, total - 1) + 1)
        return jnp.stack([one, total - one])
    sizes = jnp.asarray(length_profile(amount, total, bound, slope), jnp.int32)
    couples = (amount - 1) // 2
    giver, sink = sizes[1:1 + 2 * couples:2], sizes[2:2 + 2 * couples:2]
    margin = jnp.minimum(giver - 1, bound - sink)
    moved = jax.random.randint(jax.random.fold_in(rng, 1), (couples,), 0, 1 << 20) % (margin + 1)
    sizes = sizes.at[1:1 + 2 * couples:2].set(giver - moved).at[2:2 + 2 * couples:2].set(sink + moved)
    return sizes[jax.random.permutation(jax.random.fold_in(rng, 2), amount)]


def centred(key, shape, scale, bound, cuts=(), kind=jnp.bfloat16):
    array = scale * jax.random.normal(key, shape, jnp.float32)
    if cuts:
        array = array * steps_of(key, shape, cuts, -0.22, 0.18)
    return jnp.clip(array, -bound, bound).astype(kind)


def setup_inputs(seed: int = 0) -> dict:
    key_list = jax.random.split(jax.random.key(seed), 9)
    return {
        "hidden_in": draw_hidden_in(jax.random.fold_in(key_list[8], 71), 0),
        "out_grad": centred(key_list[1], (TOKENS, D), 1.0, 6.0, ((0, 32),)),
        "attn_saved": centred(key_list[2], (TOKENS, QW), 1.0, 6.0, ((0, 32),)),
        "row_lse": jnp.clip(2.5 + 3.5 * jax.random.uniform(key_list[3], (TOKENS, QH), jnp.float32) ** steps_of(key_list[3], (TOKENS, QH), ((0, 32),), -0.2, 0.2), 2.5, 6.0),
        "w_qkv": centred(key_list[4], (D, QW + 2 * HEAD), D ** -0.5, 0.125, ((0, 4),)),
        "w_out_t": centred(key_list[5], (D, QW), D ** -0.5, 0.125, ((0, 4),)),
        "doc_lengths": jax.vmap(lambda own: uneven_parts(own, DOCS, SEQ, SEQ // 2, 2))(jax.random.split(key_list[6], (N_FSDP * N_REP))).reshape((N_FSDP * N_REP, DOCS)).astype(jnp.int32),
        "seq_start": with_ends(jax.random.randint(key_list[7], (N_FSDP * N_REP,), 0, 8 * SEQ), jax.random.fold_in(key_list[7], 1), 0, (8 * SEQ) - 1).astype(jnp.int32),
    }


def rotary(values_in, positions, turn, head_size):
    rows = values_in.shape[0]
    heads_count = values_in.shape[1] // head_size
    half_size = head_size // 2
    inverse = 1000000.0 ** (-(jnp.arange(half_size, dtype=jnp.float32) * 2.0) / head_size)
    angles = positions.astype(jnp.float32)[:, None] * inverse[None, :]
    cosine = jnp.cos(angles)[:, None, :]
    sines = jnp.sin(angles)[:, None, :]
    shaped = values_in.reshape(rows, heads_count, head_size)
    first_half = shaped[:, :, :half_size]
    second_half = shaped[:, :, half_size:]
    result = jnp.concatenate([first_half * cosine - turn * second_half * sines, second_half * cosine + turn * first_half * sines], axis=2)
    return result.reshape(rows, heads_count * head_size)

def per_device(total, inputs):
    tokens_x, grads_y, saved, lse_rows, lengths, start, w_qkv, w_out_t = inputs
    scale = 1.0 / HEAD ** 0.5
    proj = jnp.dot(tokens_x, w_qkv, preferred_element_type=jnp.float32)
    attn_grad = jnp.dot(grads_y, w_out_t, preferred_element_type=jnp.float32).astype(jnp.bfloat16)
    positions = start + jnp.arange(SEQ, dtype=jnp.int32)
    queries = rotary(proj[:, :QW], positions, 1.0, HEAD).astype(jnp.bfloat16)
    keys = rotary(proj[:, QW:QW + HEAD], positions, 1.0, HEAD).astype(jnp.bfloat16)
    values_all = proj[:, QW + HEAD:].astype(jnp.bfloat16)
    ends = jnp.cumsum(lengths)
    local_rows = jnp.arange(SEQ, dtype=jnp.int32)
    documents = lax.optimization_barrier(jnp.sum((local_rows[:, None] >= ends[None, :]).astype(jnp.int32), axis=1))
    allowed = (documents[:, None] == documents[None, :]) & (local_rows[None, :] <= local_rows[:, None])
    key_grad = jnp.zeros((SEQ, HEAD), jnp.float32)
    value_grad = jnp.zeros((SEQ, HEAD), jnp.float32)
    query_parts = []
    for head_index in range(QH):
        lower = head_index * HEAD
        query_head = queries[:, lower:lower + HEAD]
        scores = jnp.dot(query_head, keys.T, preferred_element_type=jnp.float32) * scale
        probs = jnp.where(allowed, jnp.exp(scores - lse_rows[:, head_index:head_index + 1]), 0.0)
        grad_head = attn_grad[:, lower:lower + HEAD]
        dprobs = jnp.dot(grad_head, values_all.T, preferred_element_type=jnp.float32)
        delta = lax.optimization_barrier(jnp.sum(grad_head.astype(jnp.float32) * saved[:, lower:lower + HEAD].astype(jnp.float32), axis=1, keepdims=True))
        dscores = (probs * (dprobs - delta) * scale).astype(jnp.bfloat16)
        probs_low = probs.astype(jnp.bfloat16)
        value_grad = value_grad + jnp.dot(probs_low.T, grad_head, preferred_element_type=jnp.float32)
        query_parts.append(jnp.dot(dscores, keys, preferred_element_type=jnp.float32))
        key_grad = key_grad + jnp.dot(dscores.T, query_head, preferred_element_type=jnp.float32)
    query_grad = rotary(jnp.concatenate(query_parts, axis=1), positions, -1.0, HEAD).astype(jnp.bfloat16)
    key_grad = rotary(key_grad, positions, -1.0, HEAD).astype(jnp.bfloat16)
    d_qkv = jnp.concatenate([query_grad, key_grad, value_grad.astype(jnp.bfloat16)], axis=1)
    input_grad = jnp.dot(d_qkv, w_qkv.T, preferred_element_type=jnp.float32).astype(jnp.bfloat16)
    partial_term = jnp.concatenate([jnp.dot(tokens_x.T, d_qkv, preferred_element_type=jnp.float32), jnp.dot(grads_y.T, saved, preferred_element_type=jnp.float32)], axis=1)
    rounded = lax.optimization_barrier(partial_term.astype(jnp.bfloat16)).astype(jnp.float32)
    return (total + rounded, input_grad)

def reference(hidden_in, out_grad, attn_saved, row_lse, w_qkv, w_out_t, doc_lengths, seq_start):
    groups = doc_lengths.shape[0]

    def step_fn(total, inputs):
        return per_device(total, inputs + (w_qkv, w_out_t))
    stacked = (hidden_in.reshape(groups, SEQ, D), out_grad.reshape(groups, SEQ, D), attn_saved.reshape(groups, SEQ, QW), row_lse.reshape(groups, SEQ, QH), doc_lengths, seq_start)
    grads, input_grad = lax.scan(step_fn, jnp.zeros((D, COLS), jnp.float32), stacked)
    norm_sq = jnp.sum(grads * grads)
    grad_update = grads * lax.rsqrt(norm_sq / (D * COLS) + 1e-06)
    return (input_grad.reshape(TOKENS, D), grad_update, jnp.sqrt(norm_sq))
```

```python
import functools

import jax
import jax.numpy as jnp
import numpy as np
from jax import lax
from jax.experimental import pallas as pl
from jax.experimental.pallas import tpu as pltpu
from jax.sharding import PartitionSpec as P

HEAD = 128
MESH = pl.DeviceIdType.MESH
F32, BF16 = jnp.float32, jnp.bfloat16


def dot(a, b, ca, cb):
    return lax.dot_general(a, b, (((ca,), (cb,)), ((), ())), preferred_element_type=F32)


def flip(index, bit):
    return index + bit * (1 - 2 * ((index // bit) % 2))


def kernel(
    n_fsdp, n_rep,
    hid_hbm, og_hbm, sav_hbm, lse_hbm, wq_hbm, wo_hbm, len_ref, start_ref, freq_ref,
    ig_hbm, gu_hbm, norm_ref,
    hid, og, sav, lse, wq, wo, hid_t, og_t, proj, ag, dqkv, ig, gu,
    part, core_in, rs_in, z_mid, z_in, fin, norms, tab,
    load_sem, out_sem,
    wq_send, wq_recv, wo_send, wo_recv, wqc_send, wqc_recv, woc_send, woc_recv,
    core_send, core_recv, rs_send, rs_recv, z_send, z_recv, fin_send, fin_recv,
    norm_send, norm_recv,
):
    f = lax.axis_index("fsdp")
    r = lax.axis_index("rep")
    core, z = r % 2, r // 2
    n_z = n_rep // 2
    nb = n_fsdp.bit_length() - 1
    seq = hid.shape[0]
    chunks, _, _, half, cw = part.shape
    heads = lse.shape[1]
    qw = heads * HEAD
    wr = 2 * half
    scale = 1.0 / HEAD**0.5
    partner = (f, r + 1 - 2 * core)

    loads = []
    for k, (src, dst) in enumerate(
        [(wo_hbm, wo.at[f]), (wq_hbm, wq.at[f]), (og_hbm, og), (sav_hbm, sav), (hid_hbm, hid), (lse_hbm, lse)]
    ):
        copy = pltpu.make_async_copy(src, dst, load_sem.at[k])
        copy.start()
        loads.append(copy)

    z_near = z + 1 - 2 * (z % 2)
    z_mirror = (z // 4) * 4 + 3 - z % 4
    z_far = []
    bit = 4
    while bit < n_z:
        z_far.append(flip(z, bit))
        bit *= 2
    barrier = pltpu.get_barrier_semaphore()
    greet = [partner]
    greet += [((f + k) % n_fsdp, r) for k in range(1, n_fsdp)]
    greet += [(f, 2 * peer + core) for peer in [z_near, z_mirror] + z_far]
    for peer in greet:
        pl.semaphore_signal(barrier, inc=1, device_id=peer, device_id_type=MESH)
    pl.semaphore_wait(barrier, len(greet))

    def remote(src, dst, send, recv, device):
        return pltpu.make_async_remote_copy(
            src_ref=src, dst_ref=dst, send_sem=send, recv_sem=recv, device_id=device, device_id_type=MESH
        )

    sent = []

    def go(copy):
        copy.start()
        sent.append(copy)

    bits = [(1 - core) * (1 << s) + core * (1 << (nb - 1 - s)) for s in range(nb)]
    near = [(flip(f, b), r) for b in bits]

    def block_of(mask):
        g = f
        for s in range(nb):
            if (mask >> s) & 1:
                g = flip(g, bits[s])
        return g

    def mirror(mask):
        return sum(1 << (nb - 1 - s) for s in range(nb) if (mask >> s) & 1)

    def weight_copies(mask, message, device):
        g = block_of(mask)
        return [
            remote(ref.at[g, core], ref.at[g, core], send.at[message], recv.at[message], device)
            for ref, send, recv in ((wo, wo_send, wo_recv), (wq, wq_send, wq_recv))
        ]

    def forward(mask):
        top = mask.bit_length()
        for s in range(top, nb):
            for copy in weight_copies(mask, mask | (1 << s), near[s]):
                go(copy)

    loads[0].wait()
    loads[1].wait()
    forward(0)

    rows = lax.broadcasted_iota(jnp.int32, (seq, HEAD), 0)
    angles = (rows + start_ref[0]).astype(F32) * freq_ref[0:1, :]
    tab[0] = jnp.cos(angles)
    lanes = lax.broadcasted_iota(jnp.int32, (seq, HEAD), 1)
    sines = jnp.sin(angles)
    tab[1] = jnp.where(lanes < HEAD // 2, -sines, sines)

    def rot(v, turn):
        turned = jnp.concatenate([v[:, HEAD // 2 :], v[:, : HEAD // 2]], axis=1)
        return v * tab[0] + turn * (turned * tab[1])

    loads[2].wait()
    loads[3].wait()
    for g in range(n_fsdp):
        block = og[:, g * wr : (g + 1) * wr].T
        og_t[g, 0] = block[:half]
        og_t[g, 1] = block[half:]

    def half_for_partner(chunk, left_t, right):
        for g in range(n_fsdp):
            part[chunk, 1 - core, g] = dot(left_t[g, 1 - core], right, 1, 0).astype(BF16)
        go(remote(part.at[chunk, 1 - core], core_in.at[chunk], core_send.at[chunk], core_recv.at[chunk], partner))

    def rs_copy(chunk, mask):
        low = (mask & -mask).bit_length() - 1
        g = block_of(mask)
        return remote(
            part.at[chunk, core, g], rs_in.at[chunk, mask], rs_send.at[chunk, mask], rs_recv.at[chunk, mask], near[low]
        )

    def own_half(chunk, left_t, right):
        remote(
            part.at[chunk, 1 - core], core_in.at[chunk], core_send.at[chunk], core_recv.at[chunk], partner
        ).wait_recv()
        order = sorted(range(n_fsdp), key=lambda m: 1 - m % 2)
        for mask in order:
            g = block_of(mask)
            part[chunk, core, g] = (dot(left_t[g, core], right, 1, 0) + core_in[chunk, g].astype(F32)).astype(BF16)
            if mask & 1:
                go(rs_copy(chunk, mask))

    def rs_stage(chunk, s):
        later = [m for m in range(n_fsdp) if m % (1 << (s + 1)) == 0]
        later = sorted(later, key=lambda m: 1 - (m >> (s + 1)) % 2)
        for mask in later:
            message = mask | (1 << s)
            rs_copy(chunk, message).wait_recv()
            g = block_of(mask)
            part[chunk, core, g] = (part[chunk, core, g].astype(F32) + rs_in[chunk, message].astype(F32)).astype(BF16)
            if (mask >> (s + 1)) & 1:
                go(rs_copy(chunk, mask))

    middle = ((z % 4) + 1) // 2 % 2 == 1
    z_dev = [(f, 2 * peer + core) for peer in [z_near, z_mirror] + z_far]

    def z_up(chunk):
        return remote(part.at[chunk, core, f], z_in.at[chunk, 0], z_send.at[chunk, 0], z_recv.at[chunk, 0], z_dev[0])

    def z_across(chunk, k):
        return remote(
            z_mid.at[chunk, k], z_in.at[chunk, k + 1], z_send.at[chunk, k + 1], z_recv.at[chunk, k + 1], z_dev[k + 1]
        )

    n_across = 1 + len(z_far)

    def z_down(chunk):
        k = n_across + 1
        return remote(fin.at[chunk, core], fin.at[chunk, core], z_send.at[chunk, k], z_recv.at[chunk, k], z_dev[0])

    def fin_copy(chunk):
        return remote(fin.at[chunk, core], fin.at[chunk, core], fin_send.at[chunk], fin_recv.at[chunk], partner)

    def fin_from_partner(chunk):
        return remote(fin.at[chunk, 1 - core], fin.at[chunk, 1 - core], fin_send.at[chunk], fin_recv.at[chunk], partner)

    def z_first(chunk):
        @pl.when(middle)
        def _():
            z_up(chunk).wait_recv()
            z_mid[chunk, 0] = (part[chunk, core, f].astype(F32) + z_in[chunk, 0].astype(F32)).astype(BF16)
            z_across(chunk, 0).start()

        @pl.when(jnp.logical_not(middle))
        def _():
            z_up(chunk).start()

    def z_second(chunk):
        @pl.when(middle)
        def _():
            for k in range(n_across):
                z_across(chunk, k).wait_recv()
                total = (z_mid[chunk, k].astype(F32) + z_in[chunk, k + 1].astype(F32)).astype(BF16)
                if k + 1 < n_across:
                    z_mid[chunk, k + 1] = total
                    z_across(chunk, k + 1).start()
                else:
                    fin[chunk, core] = total
            z_down(chunk).start()

    def z_third(chunk):
        @pl.when(jnp.logical_not(middle))
        def _():
            z_down(chunk).wait_recv()

        go(fin_copy(chunk))

    def z_drain(chunk):
        @pl.when(middle)
        def _():
            for k in range(n_across):
                z_across(chunk, k).wait_send()
            z_down(chunk).wait_send()

        @pl.when(jnp.logical_not(middle))
        def _():
            z_up(chunk).wait_send()

    half_for_partner(0, og_t, sav[...])
    loads[4].wait()
    loads[5].wait()
    for g in range(n_fsdp):
        block = hid[:, g * wr : (g + 1) * wr].T
        hid_t[g, 0] = block[:half]
        hid_t[g, 1] = block[half:]

    def project(mask, first):
        g = block_of(mask)
        columns = pl.ds(pl.multiple_of(g * wr, wr), wr)
        left, other = hid[:, columns], og[:, columns]
        new = dot(left, wq[g].reshape(wr, -1), 1, 0)
        new_ag = dot(other, wo[g].reshape(wr, -1), 1, 0)
        if first:
            proj[...] = new
            ag[...] = new_ag
        else:
            proj[...] += new
            ag[...] += new_ag

    project(0, True)

    def core_copies(mask, message, side):
        g = block_of(mask)
        return [
            remote(ref.at[g, side], ref.at[g, side], send.at[message], recv.at[message], partner)
            for ref, send, recv in ((wo, woc_send, woc_recv), (wq, wqc_send, wqc_recv))
        ]

    def arrive(mask):
        top = mask.bit_length() - 1
        for copy in weight_copies(mask, mask, near[top]):
            copy.wait_recv()
        forward(mask)
        for copy in core_copies(mask, mask, core):
            go(copy)

    def use(mask):
        for copy in core_copies(mask, mirror(mask), 1 - core):
            copy.wait_recv()
        project(mask, False)

    last = n_fsdp - 1
    for mask in range(1, last):
        arrive(mask)
    for mask in range(1, last):
        use(mask)
    own_half(0, og_t, sav[...])
    arrive(last)
    use(last)

    queries = [rot(proj[:, h * HEAD : (h + 1) * HEAD], 1.0).astype(BF16) for h in range(heads)]
    keys = rot(proj[:, qw : qw + HEAD], 1.0).astype(BF16)
    values = proj[:, qw + HEAD :].astype(BF16)

    def documents(shape, axis):
        at = lax.broadcasted_iota(jnp.int32, shape, axis)
        count, end = jnp.zeros(shape, jnp.int32), 0
        for k in range(len_ref.shape[1]):
            end = end + len_ref[0, k]
            count = count + (at >= end).astype(jnp.int32)
        return at, count

    row_at, row_doc = documents((seq, seq), 0)
    col_at, col_doc = documents((seq, seq), 1)
    allowed = (row_doc == col_doc) & (col_at <= row_at)
    key_grad = jnp.zeros((seq, HEAD), F32)
    value_grad = jnp.zeros((seq, HEAD), F32)
    for h in range(heads):
        lanes_h = slice(h * HEAD, (h + 1) * HEAD)
        scores = dot(queries[h], keys, 1, 1) * scale
        probs = jnp.where(allowed, jnp.exp(scores - lse[:, h : h + 1]), 0.0)
        grad_head = ag[:, lanes_h].astype(BF16)
        dprobs = dot(grad_head, values, 1, 1)
        delta = jnp.sum(grad_head.astype(F32) * sav[:, lanes_h].astype(F32), axis=1, keepdims=True)
        dscores = (probs * (dprobs - delta) * scale).astype(BF16)
        value_grad = value_grad + dot(probs.astype(BF16), grad_head, 0, 0)
        key_grad = key_grad + dot(dscores, queries[h], 0, 0)
        dqkv[:, lanes_h] = rot(dot(dscores, keys, 1, 0), -1.0).astype(BF16)
        if h < nb:
            rs_stage(0, h)
    dqkv[:, qw : qw + HEAD] = rot(key_grad, -1.0).astype(BF16)
    dqkv[:, qw + HEAD :] = value_grad.astype(BF16)

    rest = list(range(1, chunks))
    right_of = {c: dqkv[:, (c - 1) * cw : c * cw] for c in rest}
    for c in rest:
        half_for_partner(c, hid_t, right_of[c])
    for c in rest:
        own_half(c, hid_t, right_of[c])
    for s in range(heads, nb):
        rs_stage(0, s)
    z_first(0)

    def grad_block(g):
        columns = slice(g * wr, (g + 1) * wr)
        ig[:, columns] = dot(dqkv[...], wq[g].reshape(wr, -1), 1, 1).astype(BF16)

    for g in range(n_fsdp // 2):
        grad_block(g)
    z_second(0)
    for g in range(n_fsdp // 2, n_fsdp):
        grad_block(g)
    ig_out = pltpu.make_async_copy(ig, ig_hbm, out_sem.at[0])
    ig_out.start()
    z_third(0)
    for s in range(nb):
        for c in rest:
            rs_stage(c, s)
            if s == nb - 1:
                z_first(c)
    for c in rest:
        z_second(c)
    for c in rest:
        z_third(c)

    squares = jnp.zeros((half, cw), F32)
    for c in range(chunks):
        fin_from_partner(c).wait_recv()
        low, high = fin[c, 0].astype(F32), fin[c, 1].astype(F32)
        squares = squares + low * low + high * high
    mine = jnp.sum(jnp.sum(squares, axis=0, keepdims=True), axis=1, keepdims=True)
    norms[f] = jnp.broadcast_to(mine, norms.shape[1:])
    for k in range(1, n_fsdp):
        go(remote(norms.at[f], norms.at[f], norm_send.at[k], norm_recv.at[k], ((f + k) % n_fsdp, r)))
    for k in range(1, n_fsdp):
        origin = (f + n_fsdp - k) % n_fsdp
        remote(norms.at[origin], norms.at[origin], norm_send.at[k], norm_recv.at[k], (origin, r)).wait_recv()
    total = norms[0]
    for g in range(1, n_fsdp):
        total = total + norms[g]
    norm_ref[...] = jnp.sqrt(total)
    size = n_fsdp * wr * chunks * cw
    factor = lax.rsqrt(total[0:1, 0:1] / size + 1e-06)
    for c in range(chunks):
        at = (c - 1) % chunks * cw
        for side in range(2):
            gu[side * half : (side + 1) * half, at : at + cw] = fin[c, side].astype(F32) * factor
    gu_out = pltpu.make_async_copy(gu, gu_hbm, out_sem.at[1])
    gu_out.start()
    for copy in sent:
        copy.wait_send()
    for c in range(chunks):
        z_drain(c)
    ig_out.wait()
    gu_out.wait()


def solution(mesh):
    n_fsdp, n_rep = mesh.shape["fsdp"], mesh.shape["rep"]

    def body(hidden_in, out_grad, attn_saved, row_lse, w_qkv, w_out_t, doc_lengths, seq_start):
        seq, width = hidden_in.shape
        qw, cols = attn_saved.shape[1], w_qkv.shape[1]
        wr = w_qkv.shape[0]
        half, cw = wr // 2, qw
        chunks = 1 + cols // cw
        n_across = (n_rep // 2).bit_length() - 2
        lane = np.arange(HEAD) % (HEAD // 2)
        freq = np.broadcast_to((1000000.0 ** (-2.0 * lane / HEAD)).astype(np.float32), (8, HEAD))
        dma = pltpu.SemaphoreType.DMA
        anywhere = pl.BlockSpec(memory_space=pl.ANY)
        scalar = pl.BlockSpec(memory_space=pltpu.SMEM)
        vmem = pl.BlockSpec(memory_space=pltpu.VMEM)
        F = n_fsdp
        ig, gu, norm = pl.pallas_call(
            functools.partial(kernel, n_fsdp, n_rep),
            out_shape=(
                jax.ShapeDtypeStruct((seq, width), BF16),
                jax.ShapeDtypeStruct((wr, chunks * cw), F32),
                jax.ShapeDtypeStruct((8, 128), F32),
            ),
            in_specs=[anywhere] * 6 + [scalar] * 2 + [vmem],
            out_specs=(anywhere, anywhere, vmem),
            scratch_shapes=[
                pltpu.VMEM((seq, width), BF16),
                pltpu.VMEM((seq, width), BF16),
                pltpu.VMEM((seq, qw), BF16),
                pltpu.VMEM(row_lse.shape, F32),
                pltpu.VMEM((F, 2, half, cols), BF16),
                pltpu.VMEM((F, 2, half, qw), BF16),
                pltpu.VMEM((F, 2, half, seq), BF16),
                pltpu.VMEM((F, 2, half, seq), BF16),
                pltpu.VMEM((seq, cols), F32),
                pltpu.VMEM((seq, qw), F32),
                pltpu.VMEM((seq, cols), BF16),
                pltpu.VMEM((seq, width), BF16),
                pltpu.VMEM((wr, chunks * cw), F32),
                pltpu.VMEM((chunks, 2, F, half, cw), BF16),
                pltpu.VMEM((chunks, F, half, cw), BF16),
                pltpu.VMEM((chunks, F, half, cw), BF16),
                pltpu.VMEM((chunks, n_across, half, cw), BF16),
                pltpu.VMEM((chunks, n_across + 1, half, cw), BF16),
                pltpu.VMEM((chunks, 2, half, cw), BF16),
                pltpu.VMEM((F, 8, 128), F32),
                pltpu.VMEM((2, seq, HEAD), F32),
                dma((6,)),
                dma((2,)),
            ]
            + [dma((F,))] * 8
            + [dma((chunks,))] * 2
            + [dma((chunks, F))] * 2
            + [dma((chunks, n_across + 2))] * 2
            + [dma((chunks,))] * 2
            + [dma((F,))] * 2,
            compiler_params=pltpu.CompilerParams(
                collective_id=0, has_side_effects=True, vmem_limit_bytes=56 * 2**20
            ),
        )(
            hidden_in, out_grad, attn_saved, row_lse,
            w_qkv.reshape(2, half, cols), w_out_t.reshape(2, half, qw),
            doc_lengths, seq_start, freq,
        )
        return ig, gu, norm[0, 0]

    rows = P(("fsdp", "rep"), None)
    in_specs = (rows, rows, rows, rows, P("fsdp", None), P("fsdp", None), rows, P(("fsdp", "rep")))
    return jax.shard_map(
        body, mesh=mesh, in_specs=in_specs, out_specs=(rows, P("fsdp", None), P()), check_vma=False
    )
```

```python
import functools

import jax
import jax.numpy as jnp
import numpy as np
from jax import lax
from jax.experimental import pallas as pl
from jax.experimental.pallas import tpu as pltpu
from jax.sharding import PartitionSpec as P

HEAD = 128
MESH = pl.DeviceIdType.MESH
F32, BF16 = jnp.float32, jnp.bfloat16


def dot(a, b, ca, cb):
    return lax.dot_general(a, b, (((ca,), (cb,)), ((), ())), preferred_element_type=F32)


def flip(index, bit):
    return index + bit * (1 - 2 * ((index // bit) % 2))


def kernel(
    n_fsdp, n_rep,
    hid_hbm, og_hbm, sav_hbm, lse_hbm, wq_hbm, wo_hbm, len_ref, start_ref, freq_ref,
    ig_hbm, gr_hbm, norm_ref, factor_ref,
    hid, og, sav, lse, wq, wo, hid_t, og_t, proj, ag, dqkv, ig,
    part, core_in, rs_in, z_mid, z_in, fin, norms, tab,
    load_sem, out_sem,
    wq_send, wq_recv, wo_send, wo_recv, wqc_send, wqc_recv, woc_send, woc_recv,
    core_send, core_recv, rs_send, rs_recv, z_send, z_recv, fin_send, fin_recv,
    norm_send, norm_recv,
):
    f = lax.axis_index("fsdp")
    r = lax.axis_index("rep")
    core, z = r % 2, r // 2
    n_z = n_rep // 2
    nb = n_fsdp.bit_length() - 1
    seq = hid.shape[0]
    chunks, _, _, half, cw = part.shape
    heads = lse.shape[0]
    pieces = fin_send.shape[1]
    hp = half // pieces
    qw = heads * HEAD
    wr = 2 * half
    scale = 1.0 / HEAD**0.5
    partner = (f, r + 1 - 2 * core)

    loads = []
    for k, (src, dst) in enumerate(
        [(wo_hbm, wo.at[f]), (wq_hbm, wq.at[f]), (og_hbm, og), (sav_hbm, sav), (hid_hbm, hid), (lse_hbm, lse)]
    ):
        copy = pltpu.make_async_copy(src, dst, load_sem.at[k])
        copy.start()
        loads.append(copy)

    z_near = z + 1 - 2 * (z % 2)
    z_mirror = (z // 4) * 4 + 3 - z % 4
    z_far = []
    bit = 4
    while bit < n_z:
        z_far.append(flip(z, bit))
        bit *= 2
    barrier = pltpu.get_barrier_semaphore()
    greet = [partner]
    greet += [((f + k) % n_fsdp, 2 * z + side) for k in range(1, n_fsdp) for side in range(2)]
    greet += [(f, 2 * peer + core) for peer in [z_near, z_mirror] + z_far]
    for peer in greet:
        pl.semaphore_signal(barrier, inc=1, device_id=peer, device_id_type=MESH)
    pl.semaphore_wait(barrier, len(greet))

    def remote(src, dst, send, recv, device):
        return pltpu.make_async_remote_copy(
            src_ref=src, dst_ref=dst, send_sem=send, recv_sem=recv, device_id=device, device_id_type=MESH
        )

    sent = []

    def go(copy):
        copy.start()
        sent.append(copy)

    bits = [(1 - core) * (1 << s) + core * (1 << (nb - 1 - s)) for s in range(nb)]
    near = [(flip(f, b), r) for b in bits]

    def block_of(mask):
        g = f
        for s in range(nb):
            if (mask >> s) & 1:
                g = flip(g, bits[s])
        return g

    def mirror(mask):
        return sum(1 << (nb - 1 - s) for s in range(nb) if (mask >> s) & 1)

    def weight_copies(mask, message, device):
        g = block_of(mask)
        return [
            remote(ref.at[g, core], ref.at[g, core], send.at[message], recv.at[message], device)
            for ref, send, recv in ((wo, wo_send, wo_recv), (wq, wq_send, wq_recv))
        ]

    def forward(mask):
        top = mask.bit_length()
        for s in range(top, nb):
            for copy in weight_copies(mask, mask | (1 << s), near[s]):
                go(copy)

    loads[0].wait()
    loads[1].wait()
    forward(0)

    rows = lax.broadcasted_iota(jnp.int32, (seq, HEAD), 0)
    angles = (rows + start_ref[0]).astype(F32) * freq_ref[0:1, :]
    tab[0] = jnp.cos(angles)
    lanes = lax.broadcasted_iota(jnp.int32, (seq, HEAD), 1)
    sines = jnp.sin(angles)
    tab[1] = jnp.where(lanes < HEAD // 2, -sines, sines)

    def rot(v, turn):
        turned = jnp.concatenate([v[:, HEAD // 2 :], v[:, : HEAD // 2]], axis=1)
        return v * tab[0] + turn * (turned * tab[1])

    loads[2].wait()
    loads[3].wait()
    for g in range(n_fsdp):
        block = og[:, g * wr : (g + 1) * wr].T
        og_t[g, 0] = block[:half]
        og_t[g, 1] = block[half:]

    def half_for_partner(chunk, left_t, right):
        for g in range(n_fsdp):
            part[chunk, 1 - core, g] = dot(left_t[g, 1 - core], right, 1, 0).astype(BF16)
        go(remote(part.at[chunk, 1 - core], core_in.at[chunk], core_send.at[chunk], core_recv.at[chunk], partner))

    def rows_of(p):
        return pl.ds(p * hp, hp)

    def rs_copy(chunk, p, mask):
        low = (mask & -mask).bit_length() - 1
        return remote(
            part.at[chunk, core, block_of(mask), rows_of(p)],
            rs_in.at[chunk, mask, rows_of(p)],
            rs_send.at[chunk, p, mask],
            rs_recv.at[chunk, p, mask],
            near[low],
        )

    def own_half(chunk, left_t, right, send=True):
        remote(
            part.at[chunk, 1 - core], core_in.at[chunk], core_send.at[chunk], core_recv.at[chunk], partner
        ).wait_recv()

        def term(mask):
            g = block_of(mask)
            part[chunk, core, g] = (dot(left_t[g, core], right, 1, 0) + core_in[chunk, g].astype(F32)).astype(BF16)

        for mask in range(n_fsdp - 1, 0, -2):
            term(mask)
        if send:
            send_first(chunk)
        for mask in range(n_fsdp - 2, -1, -2):
            term(mask)

    def send_first(chunk):
        for p in range(pieces):
            for mask in range(n_fsdp - 1, 0, -2):
                go(rs_copy(chunk, p, mask))

    def rs_stage(chunk, p, s):
        later = [m for m in range(n_fsdp) if m % (1 << (s + 1)) == 0]
        later = sorted(later, key=lambda m: 1 - (m >> (s + 1)) % 2)
        for mask in later:
            message = mask | (1 << s)
            rs_copy(chunk, p, message).wait_recv()
            g = block_of(mask)
            at = rows_of(p)
            part[chunk, core, g, at] = (
                part[chunk, core, g, at].astype(F32) + rs_in[chunk, message, at].astype(F32)
            ).astype(BF16)
            if (mask >> (s + 1)) & 1:
                go(rs_copy(chunk, p, mask))

    middle = ((z % 4) + 1) // 2 % 2 == 1
    z_dev = [(f, 2 * peer + core) for peer in [z_near, z_mirror] + z_far]

    def z_copy(chunk, p, k, src, dst, device):
        return remote(src, dst, z_send.at[chunk, p, k], z_recv.at[chunk, p, k], device)

    def z_up(chunk, p):
        at = rows_of(p)
        return z_copy(chunk, p, 0, part.at[chunk, core, f, at], z_in.at[chunk, 0, at], z_dev[0])

    def z_across(chunk, p, k):
        at = rows_of(p)
        return z_copy(chunk, p, k + 1, z_mid.at[chunk, k, at], z_in.at[chunk, k + 1, at], z_dev[k + 1])

    n_across = 1 + len(z_far)

    def z_down(chunk, p):
        ref = fin.at[chunk, core, rows_of(p)]
        return z_copy(chunk, p, n_across + 1, ref, ref, z_dev[0])

    def fin_copy(chunk, p, side):
        ref = fin.at[chunk, side, rows_of(p)]
        return remote(ref, ref, fin_send.at[chunk, p], fin_recv.at[chunk, p], partner)

    def z_first(chunk, p):
        at = rows_of(p)

        @pl.when(middle)
        def _():
            z_up(chunk, p).wait_recv()
            z_mid[chunk, 0, at] = (part[chunk, core, f, at].astype(F32) + z_in[chunk, 0, at].astype(F32)).astype(BF16)
            z_across(chunk, p, 0).start()

    def z_start(chunk, p):
        @pl.when(jnp.logical_not(middle))
        def _():
            z_up(chunk, p).start()

    def z_second(chunk, p):
        at = rows_of(p)

        @pl.when(middle)
        def _():
            for k in range(n_across):
                z_across(chunk, p, k).wait_recv()
                total = (z_mid[chunk, k, at].astype(F32) + z_in[chunk, k + 1, at].astype(F32)).astype(BF16)
                if k + 1 < n_across:
                    z_mid[chunk, k + 1, at] = total
                    z_across(chunk, p, k + 1).start()
                else:
                    fin[chunk, core, at] = total
            z_down(chunk, p).start()

    squares = [jnp.zeros((8, cw), F32)]

    def z_third(chunk, p):
        @pl.when(jnp.logical_not(middle))
        def _():
            z_down(chunk, p).wait_recv()

        go(fin_copy(chunk, p, core))
        own = fin[chunk, core, rows_of(p)].astype(F32)
        squares[0] = squares[0] + jnp.sum((own * own).reshape(hp // 8, 8, cw), axis=0)

    def z_drain(chunk, p):
        @pl.when(middle)
        def _():
            for k in range(n_across):
                z_across(chunk, p, k).wait_send()
            z_down(chunk, p).wait_send()

        @pl.when(jnp.logical_not(middle))
        def _():
            z_up(chunk, p).wait_send()

    every = range(pieces)

    half_for_partner(0, og_t, sav[...])
    loads[4].wait()
    loads[5].wait()
    for g in range(n_fsdp):
        block = hid[:, g * wr : (g + 1) * wr].T
        hid_t[g, 0] = block[:half]
        hid_t[g, 1] = block[half:]

    def project(mask, first):
        g = block_of(mask)
        columns = pl.ds(pl.multiple_of(g * wr, wr), wr)
        left, other = hid[:, columns], og[:, columns]
        new = dot(left, wq[g].reshape(wr, -1), 1, 0)
        new_ag = dot(other, wo[g].reshape(wr, -1), 1, 0)
        if first:
            proj[...] = new
            ag[...] = new_ag
        else:
            proj[...] += new
            ag[...] += new_ag

    project(0, True)

    def core_copies(mask, message, side):
        g = block_of(mask)
        return [
            remote(ref.at[g, side], ref.at[g, side], send.at[message], recv.at[message], partner)
            for ref, send, recv in ((wo, woc_send, woc_recv), (wq, wqc_send, wqc_recv))
        ]

    def arrive(mask):
        top = mask.bit_length() - 1
        for copy in weight_copies(mask, mask, near[top]):
            copy.wait_recv()
        forward(mask)
        for copy in core_copies(mask, mask, core):
            go(copy)

    def use(mask):
        for copy in core_copies(mask, mirror(mask), 1 - core):
            copy.wait_recv()
        project(mask, False)

    last = n_fsdp - 1
    for mask in range(1, last):
        arrive(mask)
    for mask in range(1, last):
        use(mask)
    own_half(0, og_t, sav[...], False)
    arrive(last)
    send_first(0)
    use(last)
    lse_rows = jnp.concatenate([lse[...]] * (8 // heads), axis=0).T

    queries = [rot(proj[:, h * HEAD : (h + 1) * HEAD], 1.0).astype(BF16) for h in range(heads)]
    keys = rot(proj[:, qw : qw + HEAD], 1.0).astype(BF16)
    values = proj[:, qw + HEAD :].astype(BF16)

    def documents(shape, axis):
        at = lax.broadcasted_iota(jnp.int32, shape, axis)
        count, end = jnp.zeros(shape, jnp.int32), 0
        for k in range(len_ref.shape[1]):
            end = end + len_ref[0, k]
            count = count + (at >= end).astype(jnp.int32)
        return at, count

    row_at, row_doc = documents((seq, seq), 0)
    col_at, col_doc = documents((seq, seq), 1)
    allowed = (row_doc == col_doc) & (col_at <= row_at)
    key_grad = jnp.zeros((seq, HEAD), F32)
    value_grad = jnp.zeros((seq, HEAD), F32)
    for h in range(heads):
        lanes_h = slice(h * HEAD, (h + 1) * HEAD)
        scores = dot(queries[h], keys, 1, 1) * scale
        probs = jnp.where(allowed, jnp.exp(scores - lse_rows[:, h : h + 1]), 0.0)
        grad_head = ag[:, lanes_h].astype(BF16)
        dprobs = dot(grad_head, values, 1, 1)
        delta = jnp.sum(grad_head.astype(F32) * sav[:, lanes_h].astype(F32), axis=1, keepdims=True)
        dscores = (probs * (dprobs - delta) * scale).astype(BF16)
        value_grad = value_grad + dot(probs.astype(BF16), grad_head, 0, 0)
        key_grad = key_grad + dot(dscores, queries[h], 0, 0)
        dqkv[:, lanes_h] = rot(dot(dscores, keys, 1, 0), -1.0).astype(BF16)
    dqkv[:, qw : qw + HEAD] = rot(key_grad, -1.0).astype(BF16)
    dqkv[:, qw + HEAD :] = value_grad.astype(BF16)

    rest = list(range(1, chunks))
    right_of = {c: dqkv[:, (c - 1) * cw : c * cw] for c in rest}
    for c in rest:
        half_for_partner(c, hid_t, right_of[c])
    for p in every:
        rs_stage(0, p, 0)
    for c in rest:
        own_half(c, hid_t, right_of[c])
    for s in range(1, nb):
        for p in every:
            rs_stage(0, p, s)
    for p in every:
        z_start(0, p)

    def grad_block(g):
        columns = slice(g * wr, (g + 1) * wr)
        ig[:, columns] = dot(dqkv[...], wq[g].reshape(wr, -1), 1, 1).astype(BF16)

    ig_out = pltpu.make_async_copy(ig, ig_hbm, out_sem.at[0])
    items = [(c, p) for c in rest for p in every]
    depth = nb + 3

    def advance(c, p, s):
        if s < nb:
            rs_stage(c, p, s)
            if s == nb - 1:
                z_start(c, p)
        elif s == nb:
            z_first(c, p)
        elif s == nb + 1:
            z_second(c, p)
        else:
            z_third(c, p)

    for t in range(len(items) + depth - 1):
        if t < n_fsdp:
            grad_block(t)
        if t == n_fsdp - 1:
            ig_out.start()
        if t < 3:
            for p in every:
                advance(0, p, nb + t)
        for k in range(max(0, t - depth + 1), min(t, len(items) - 1) + 1):
            advance(*items[k], t - k)
    for t in range(len(items) + depth - 1, n_fsdp):
        grad_block(t)
    if n_fsdp > len(items) + depth - 1:
        ig_out.start()

    mine = jnp.sum(jnp.sum(squares[0], axis=0, keepdims=True), axis=1, keepdims=True)
    slot = 2 * f + core
    norms[slot] = jnp.broadcast_to(mine, norms.shape[1:])
    rounds = [(k, side) for k in range(n_fsdp) for side in range(2) if k or side]

    def norm_copy(k, side, place, sign):
        at = 2 * k + side
        column = (f + sign * k + n_fsdp) % n_fsdp
        row = 2 * z + (core + side) % 2
        return remote(norms.at[place], norms.at[place], norm_send.at[at], norm_recv.at[at], (column, row))

    for k, side in rounds:
        go(norm_copy(k, side, slot, 1))
    gr_outs = []
    for c in range(chunks):
        for p in every:
            fin_copy(c, p, 1 - core).wait_recv()
        for side in range(2):
            columns = pl.ds((c - 1) % chunks * cw, cw)
            out = pltpu.make_async_copy(
                fin.at[c, side], gr_hbm.at[pl.ds(side * half, half), columns], out_sem.at[1 + 2 * c + side]
            )
            out.start()
            gr_outs.append(out)
    for k, side in rounds:
        norm_copy(k, side, 2 * ((f - k + n_fsdp) % n_fsdp) + (core + side) % 2, -1).wait_recv()
    total = norms[0]
    for k in range(1, 2 * n_fsdp):
        total = total + norms[k]
    size = n_fsdp * wr * chunks * cw
    norm_ref[0, 0] = jnp.max(jnp.sqrt(total))
    factor_ref[0, 0] = jnp.max(lax.rsqrt(total / size + 1e-06))
    for copy in sent:
        copy.wait_send()
    for c in range(chunks):
        for p in every:
            z_drain(c, p)
    ig_out.wait()
    for out in gr_outs:
        out.wait()


def solution(mesh):
    n_fsdp, n_rep = mesh.shape["fsdp"], mesh.shape["rep"]

    def body(hidden_in, out_grad, attn_saved, row_lse, w_qkv, w_out_t, doc_lengths, seq_start):
        seq, width = hidden_in.shape
        qw, cols = attn_saved.shape[1], w_qkv.shape[1]
        wr = w_qkv.shape[0]
        half, cw = wr // 2, qw
        chunks = 1 + cols // cw
        n_across = (n_rep // 2).bit_length() - 2
        lane = np.arange(HEAD) % (HEAD // 2)
        freq = np.broadcast_to((1000000.0 ** (-2.0 * lane / HEAD)).astype(np.float32), (1, HEAD))
        dma = pltpu.SemaphoreType.DMA
        anywhere = pl.BlockSpec(memory_space=pl.ANY)
        scalar = pl.BlockSpec(memory_space=pltpu.SMEM)
        vmem = pl.BlockSpec(memory_space=pltpu.VMEM)
        F = n_fsdp
        pieces = 4
        ig, grads, norm, factor = pl.pallas_call(
            functools.partial(kernel, n_fsdp, n_rep),
            out_shape=(
                jax.ShapeDtypeStruct((seq, width), BF16),
                jax.ShapeDtypeStruct((wr, chunks * cw), BF16),
                jax.ShapeDtypeStruct((1, 1), F32),
                jax.ShapeDtypeStruct((1, 1), F32),
            ),
            in_specs=[anywhere] * 6 + [scalar] * 2 + [vmem],
            out_specs=(anywhere, anywhere, scalar, scalar),
            scratch_shapes=[
                pltpu.VMEM((seq, width), BF16),
                pltpu.VMEM((seq, width), BF16),
                pltpu.VMEM((seq, qw), BF16),
                pltpu.VMEM(row_lse.shape[::-1], F32),
                pltpu.VMEM((F, 2, half, cols), BF16),
                pltpu.VMEM((F, 2, half, qw), BF16),
                pltpu.VMEM((F, 2, half, seq), BF16),
                pltpu.VMEM((F, 2, half, seq), BF16),
                pltpu.VMEM((seq, cols), F32),
                pltpu.VMEM((seq, qw), F32),
                pltpu.VMEM((seq, cols), BF16),
                pltpu.VMEM((seq, width), BF16),
                pltpu.VMEM((chunks, 2, F, half, cw), BF16),
                pltpu.VMEM((chunks, F, half, cw), BF16),
                pltpu.VMEM((chunks, F, half, cw), BF16),
                pltpu.VMEM((chunks, n_across, half, cw), BF16),
                pltpu.VMEM((chunks, n_across + 1, half, cw), BF16),
                pltpu.VMEM((chunks, 2, half, cw), BF16),
                pltpu.VMEM((2 * F, 8, 128), F32),
                pltpu.VMEM((2, seq, HEAD), F32),
                dma((6,)),
                dma((1 + 2 * chunks,)),
            ]
            + [dma((F,))] * 8
            + [dma((chunks,))] * 2
            + [dma((chunks, pieces, F))] * 2
            + [dma((chunks, pieces, n_across + 2))] * 2
            + [dma((chunks, pieces))] * 2
            + [dma((2 * F,))] * 2,
            compiler_params=pltpu.CompilerParams(
                collective_id=0, has_side_effects=True, vmem_limit_bytes=56 * 2**20
            ),
        )(
            hidden_in, out_grad, attn_saved, row_lse.T,
            w_qkv.reshape(2, half, cols), w_out_t.reshape(2, half, qw),
            doc_lengths, seq_start, freq,
        )
        return ig, grads.astype(F32) * factor[0, 0], norm[0, 0]

    rows = P(("fsdp", "rep"), None)
    in_specs = (rows, rows, rows, rows, P("fsdp", None), P("fsdp", None), rows, P(("fsdp", "rep")))
    return jax.shard_map(
        body, mesh=mesh, in_specs=in_specs, out_specs=(rows, P("fsdp", None), P()), check_vma=False
    )
```

```python
import functools

import jax
import jax.numpy as jnp
import numpy as np
from jax import lax
from jax.experimental import pallas as pl
from jax.experimental.pallas import tpu as pltpu
from jax.sharding import PartitionSpec as P

HEAD = 128
MESH = pl.DeviceIdType.MESH
F32, BF16 = jnp.float32, jnp.bfloat16


def dot(a, b, ca, cb):
    return lax.dot_general(a, b, (((ca,), (cb,)), ((), ())), preferred_element_type=F32)


def flip(index, bit):
    return index + bit * (1 - 2 * ((index // bit) % 2))


def kernel(
    n_fsdp, n_rep,
    hid_hbm, og_hbm, sav_hbm, lse_hbm, wq_hbm, wo_hbm, len_ref, start_ref, freq_ref,
    ig_hbm, gr_hbm, norm_ref, factor_ref,
    hid, og, sav, lse, wq, wo, hid_t, og_t, proj, ag, dqkv, ig,
    part, core_in, rs_in, z_mid, z_in, fin, norms, tab,
    load_sem, out_sem,
    wq_send, wq_recv, wo_send, wo_recv, wqc_send, wqc_recv, woc_send, woc_recv,
    core_send, core_recv, rs_send, rs_recv, z_send, z_recv, fin_send, fin_recv,
    norm_send, norm_recv,
):
    f = lax.axis_index("fsdp")
    r = lax.axis_index("rep")
    core, z = r % 2, r // 2
    n_z = n_rep // 2
    nb = n_fsdp.bit_length() - 1
    seq = hid.shape[0]
    chunks, _, _, half, cw = part.shape
    heads = lse.shape[0]
    pieces = fin_send.shape[1]
    hp = half // pieces
    qw = heads * HEAD
    wr = 2 * half
    scale = 1.0 / HEAD**0.5
    partner = (f, r + 1 - 2 * core)

    loads = []
    for k, (src, dst) in enumerate(
        [(wo_hbm, wo.at[f]), (wq_hbm, wq.at[f]), (og_hbm, og), (sav_hbm, sav), (hid_hbm, hid), (lse_hbm, lse)]
    ):
        copy = pltpu.make_async_copy(src, dst, load_sem.at[k])
        copy.start()
        loads.append(copy)

    z_near = z + 1 - 2 * (z % 2)
    z_mirror = (z // 4) * 4 + 3 - z % 4
    z_far = []
    bit = 4
    while bit < n_z:
        z_far.append(flip(z, bit))
        bit *= 2
    barrier = pltpu.get_barrier_semaphore()
    greet = [partner]
    greet += [((f + k) % n_fsdp, 2 * z + side) for k in range(1, n_fsdp) for side in range(2)]
    greet += [(f, 2 * peer + core) for peer in [z_near, z_mirror] + z_far]
    for peer in greet:
        pl.semaphore_signal(barrier, inc=1, device_id=peer, device_id_type=MESH)
    pl.semaphore_wait(barrier, len(greet))

    def remote(src, dst, send, recv, device):
        return pltpu.make_async_remote_copy(
            src_ref=src, dst_ref=dst, send_sem=send, recv_sem=recv, device_id=device, device_id_type=MESH
        )

    sent = []

    def go(copy):
        copy.start()
        sent.append(copy)

    bits = [(1 - core) * (1 << s) + core * (1 << (nb - 1 - s)) for s in range(nb)]
    near = [(flip(f, b), r) for b in bits]

    def block_of(mask):
        g = f
        for s in range(nb):
            if (mask >> s) & 1:
                g = flip(g, bits[s])
        return g

    def mirror(mask):
        return sum(1 << (nb - 1 - s) for s in range(nb) if (mask >> s) & 1)

    def weight_copies(mask, message, device):
        g = block_of(mask)
        return [
            remote(ref.at[g, core], ref.at[g, core], send.at[message], recv.at[message], device)
            for ref, send, recv in ((wo, wo_send, wo_recv), (wq, wq_send, wq_recv))
        ]

    def forward(mask):
        top = mask.bit_length()
        for s in range(top, nb):
            for copy in weight_copies(mask, mask | (1 << s), near[s]):
                go(copy)

    loads[0].wait()
    loads[1].wait()
    forward(0)

    rows = lax.broadcasted_iota(jnp.int32, (seq, HEAD), 0)
    angles = (rows + start_ref[0]).astype(F32) * freq_ref[0:1, :]
    tab[0] = jnp.cos(angles)
    lanes = lax.broadcasted_iota(jnp.int32, (seq, HEAD), 1)
    sines = jnp.sin(angles)
    tab[1] = jnp.where(lanes < HEAD // 2, -sines, sines)

    def rot(v, turn):
        turned = jnp.concatenate([v[:, HEAD // 2 :], v[:, : HEAD // 2]], axis=1)
        return v * tab[0] + turn * (turned * tab[1])

    loads[2].wait()
    loads[3].wait()
    for g in range(n_fsdp):
        block = og[:, g * wr : (g + 1) * wr].T
        og_t[g, 0] = block[:half]
        og_t[g, 1] = block[half:]

    def half_for_partner(chunk, left_t, right):
        for g in range(n_fsdp):
            part[chunk, 1 - core, g] = dot(left_t[g, 1 - core], right, 1, 0).astype(BF16)
        go(remote(part.at[chunk, 1 - core], core_in.at[chunk], core_send.at[chunk], core_recv.at[chunk], partner))

    def rows_of(p):
        return pl.ds(p * hp, hp)

    def rs_copy(chunk, p, mask):
        low = (mask & -mask).bit_length() - 1
        return remote(
            part.at[chunk, core, block_of(mask), rows_of(p)],
            rs_in.at[chunk, mask, rows_of(p)],
            rs_send.at[chunk, p, mask],
            rs_recv.at[chunk, p, mask],
            near[low],
        )

    def own_half(chunk, left_t, right, send=True):
        remote(
            part.at[chunk, 1 - core], core_in.at[chunk], core_send.at[chunk], core_recv.at[chunk], partner
        ).wait_recv()

        def term(mask):
            g = block_of(mask)
            part[chunk, core, g] = (dot(left_t[g, core], right, 1, 0) + core_in[chunk, g].astype(F32)).astype(BF16)

        for mask in range(n_fsdp - 1, 0, -2):
            term(mask)
        if send:
            send_first(chunk)
        for mask in range(n_fsdp - 2, -1, -2):
            term(mask)

    def send_first(chunk):
        for p in range(pieces):
            for mask in range(n_fsdp - 1, 0, -2):
                go(rs_copy(chunk, p, mask))

    def rs_stage(chunk, p, s):
        later = [m for m in range(n_fsdp) if m % (1 << (s + 1)) == 0]
        later = sorted(later, key=lambda m: 1 - (m >> (s + 1)) % 2)
        for mask in later:
            message = mask | (1 << s)
            rs_copy(chunk, p, message).wait_recv()
            g = block_of(mask)
            at = rows_of(p)
            part[chunk, core, g, at] = (
                part[chunk, core, g, at].astype(F32) + rs_in[chunk, message, at].astype(F32)
            ).astype(BF16)
            if (mask >> (s + 1)) & 1:
                go(rs_copy(chunk, p, mask))

    middle = ((z % 4) + 1) // 2 % 2 == 1
    z_dev = [(f, 2 * peer + core) for peer in [z_near, z_mirror] + z_far]

    def z_copy(chunk, p, k, src, dst, device):
        return remote(src, dst, z_send.at[chunk, p, k], z_recv.at[chunk, p, k], device)

    def z_up(chunk, p):
        at = rows_of(p)
        return z_copy(chunk, p, 0, part.at[chunk, core, f, at], z_in.at[chunk, 0, at], z_dev[0])

    def z_across(chunk, p, k):
        at = rows_of(p)
        return z_copy(chunk, p, k + 1, z_mid.at[chunk, k, at], z_in.at[chunk, k + 1, at], z_dev[k + 1])

    n_across = 1 + len(z_far)

    def z_down(chunk, p):
        ref = fin.at[chunk, core, rows_of(p)]
        return z_copy(chunk, p, n_across + 1, ref, ref, z_dev[0])

    def fin_copy(chunk, p, side):
        ref = fin.at[chunk, side, rows_of(p)]
        return remote(ref, ref, fin_send.at[chunk, p], fin_recv.at[chunk, p], partner)

    def z_first(chunk, p):
        at = rows_of(p)

        @pl.when(middle)
        def _():
            z_up(chunk, p).wait_recv()
            z_mid[chunk, 0, at] = (part[chunk, core, f, at].astype(F32) + z_in[chunk, 0, at].astype(F32)).astype(BF16)
            z_across(chunk, p, 0).start()

    def z_start(chunk, p):
        @pl.when(jnp.logical_not(middle))
        def _():
            z_up(chunk, p).start()

    def z_second(chunk, p):
        at = rows_of(p)

        @pl.when(middle)
        def _():
            for k in range(n_across):
                z_across(chunk, p, k).wait_recv()
                total = (z_mid[chunk, k, at].astype(F32) + z_in[chunk, k + 1, at].astype(F32)).astype(BF16)
                if k + 1 < n_across:
                    z_mid[chunk, k + 1, at] = total
                    z_across(chunk, p, k + 1).start()
                else:
                    fin[chunk, core, at] = total
            z_down(chunk, p).start()

    squares = [jnp.zeros((8, cw), F32)]

    def z_third(chunk, p):
        @pl.when(jnp.logical_not(middle))
        def _():
            z_down(chunk, p).wait_recv()

        go(fin_copy(chunk, p, core))
        own = fin[chunk, core, rows_of(p)].astype(F32)
        squares[0] = squares[0] + jnp.sum((own * own).reshape(hp // 8, 8, cw), axis=0)

    def z_drain(chunk, p):
        @pl.when(middle)
        def _():
            for k in range(n_across):
                z_across(chunk, p, k).wait_send()
            z_down(chunk, p).wait_send()

        @pl.when(jnp.logical_not(middle))
        def _():
            z_up(chunk, p).wait_send()

    every = range(pieces)

    half_for_partner(0, og_t, sav[...])
    loads[4].wait()
    loads[5].wait()
    for g in range(n_fsdp):
        block = hid[:, g * wr : (g + 1) * wr].T
        hid_t[g, 0] = block[:half]
        hid_t[g, 1] = block[half:]

    def project(mask, first):
        g = block_of(mask)
        columns = pl.ds(pl.multiple_of(g * wr, wr), wr)
        left, other = hid[:, columns], og[:, columns]
        new = dot(left, wq[g].reshape(wr, -1), 1, 0)
        new_ag = dot(other, wo[g].reshape(wr, -1), 1, 0)
        if first:
            proj[...] = new
            ag[...] = new_ag
        else:
            proj[...] += new
            ag[...] += new_ag

    project(0, True)

    def core_copies(mask, message, side):
        g = block_of(mask)
        return [
            remote(ref.at[g, side], ref.at[g, side], send.at[message], recv.at[message], partner)
            for ref, send, recv in ((wo, woc_send, woc_recv), (wq, wqc_send, wqc_recv))
        ]

    def arrive(mask):
        top = mask.bit_length() - 1
        for copy in weight_copies(mask, mask, near[top]):
            copy.wait_recv()
        forward(mask)
        for copy in core_copies(mask, mask, core):
            go(copy)

    def use(mask):
        for copy in core_copies(mask, mirror(mask), 1 - core):
            copy.wait_recv()
        project(mask, False)

    last = n_fsdp - 1
    for mask in range(1, last):
        arrive(mask)
    for mask in range(1, last):
        use(mask)
    own_half(0, og_t, sav[...], False)
    arrive(last)
    send_first(0)
    use(last)
    lse_rows = jnp.concatenate([lse[...]] * (8 // heads), axis=0).T

    queries = [rot(proj[:, h * HEAD : (h + 1) * HEAD], 1.0).astype(BF16) for h in range(heads)]
    keys = rot(proj[:, qw : qw + HEAD], 1.0).astype(BF16)
    values = proj[:, qw + HEAD :].astype(BF16)

    def documents(shape, axis):
        at = lax.broadcasted_iota(jnp.int32, shape, axis)
        count, end = jnp.zeros(shape, jnp.int32), 0
        for k in range(len_ref.shape[1]):
            end = end + len_ref[0, k]
            count = count + (at >= end).astype(jnp.int32)
        return at, count

    row_at, row_doc = documents((seq, seq), 0)
    col_at, col_doc = documents((seq, seq), 1)
    allowed = (row_doc == col_doc) & (col_at <= row_at)
    key_grad = jnp.zeros((seq, HEAD), F32)
    value_grad = jnp.zeros((seq, HEAD), F32)
    for h in range(heads):
        lanes_h = slice(h * HEAD, (h + 1) * HEAD)
        scores = dot(queries[h], keys, 1, 1) * scale
        probs = jnp.where(allowed, jnp.exp(scores - lse_rows[:, h : h + 1]), 0.0)
        grad_head = ag[:, lanes_h].astype(BF16)
        dprobs = dot(grad_head, values, 1, 1)
        delta = jnp.sum(grad_head.astype(F32) * sav[:, lanes_h].astype(F32), axis=1, keepdims=True)
        dscores = (probs * (dprobs - delta) * scale).astype(BF16)
        value_grad = value_grad + dot(probs.astype(BF16), grad_head, 0, 0)
        key_grad = key_grad + dot(dscores, queries[h], 0, 0)
        dqkv[:, lanes_h] = rot(dot(dscores, keys, 1, 0), -1.0).astype(BF16)
    dqkv[:, qw : qw + HEAD] = rot(key_grad, -1.0).astype(BF16)
    dqkv[:, qw + HEAD :] = value_grad.astype(BF16)

    rest = list(range(1, chunks))
    right_of = {c: dqkv[:, (c - 1) * cw : c * cw] for c in rest}
    for c in rest:
        half_for_partner(c, hid_t, right_of[c])
    for p in every:
        rs_stage(0, p, 0)
    for c in rest:
        own_half(c, hid_t, right_of[c])
    for s in range(1, nb):
        for p in every:
            rs_stage(0, p, s)
    for p in every:
        z_start(0, p)

    def grad_block(g):
        columns = slice(g * wr, (g + 1) * wr)
        ig[:, columns] = dot(dqkv[...], wq[g].reshape(wr, -1), 1, 1).astype(BF16)

    ig_out = pltpu.make_async_copy(ig, ig_hbm, out_sem.at[0])
    items = [(c, p) for c in rest for p in every]
    depth = nb + 3

    def advance(c, p, s):
        if s < nb:
            rs_stage(c, p, s)
            if s == nb - 1:
                z_start(c, p)
        elif s == nb:
            z_first(c, p)
        elif s == nb + 1:
            z_second(c, p)
        else:
            z_third(c, p)

    for t in range(depth):
        if t < n_fsdp:
            grad_block(t)
        if t == n_fsdp - 1:
            ig_out.start()
        if t < 3:
            for p in every:
                advance(0, p, nb + t)
        for c, p in items:
            advance(c, p, t)
    for t in range(depth, n_fsdp):
        grad_block(t)
    if n_fsdp > depth:
        ig_out.start()

    mine = jnp.sum(jnp.sum(squares[0], axis=0, keepdims=True), axis=1, keepdims=True)
    slot = 2 * f + core
    norms[slot] = jnp.broadcast_to(mine, norms.shape[1:])
    rounds = [(k, side) for k in range(n_fsdp) for side in range(2) if k or side]

    def norm_copy(k, side, place, sign):
        at = 2 * k + side
        column = (f + sign * k + n_fsdp) % n_fsdp
        row = 2 * z + (core + side) % 2
        return remote(norms.at[place], norms.at[place], norm_send.at[at], norm_recv.at[at], (column, row))

    for k, side in rounds:
        go(norm_copy(k, side, slot, 1))
    gr_outs = []
    for c in range(chunks):
        for p in every:
            fin_copy(c, p, 1 - core).wait_recv()
        for side in range(2):
            columns = pl.ds((c - 1) % chunks * cw, cw)
            out = pltpu.make_async_copy(
                fin.at[c, side], gr_hbm.at[pl.ds(side * half, half), columns], out_sem.at[1 + 2 * c + side]
            )
            out.start()
            gr_outs.append(out)
    for k, side in rounds:
        norm_copy(k, side, 2 * ((f - k + n_fsdp) % n_fsdp) + (core + side) % 2, -1).wait_recv()
    total = norms[0]
    for k in range(1, 2 * n_fsdp):
        total = total + norms[k]
    size = n_fsdp * wr * chunks * cw
    norm_ref[0, 0] = jnp.max(jnp.sqrt(total))
    factor_ref[0, 0] = jnp.max(lax.rsqrt(total / size + 1e-06))
    for copy in sent:
        copy.wait_send()
    for c in range(chunks):
        for p in every:
            z_drain(c, p)
    ig_out.wait()
    for out in gr_outs:
        out.wait()


def solution(mesh):
    n_fsdp, n_rep = mesh.shape["fsdp"], mesh.shape["rep"]

    def body(hidden_in, out_grad, attn_saved, row_lse, w_qkv, w_out_t, doc_lengths, seq_start):
        seq, width = hidden_in.shape
        qw, cols = attn_saved.shape[1], w_qkv.shape[1]
        wr = w_qkv.shape[0]
        half, cw = wr // 2, qw
        chunks = 1 + cols // cw
        n_across = (n_rep // 2).bit_length() - 2
        lane = np.arange(HEAD) % (HEAD // 2)
        freq = np.broadcast_to((1000000.0 ** (-2.0 * lane / HEAD)).astype(np.float32), (1, HEAD))
        dma = pltpu.SemaphoreType.DMA
        anywhere = pl.BlockSpec(memory_space=pl.ANY)
        scalar = pl.BlockSpec(memory_space=pltpu.SMEM)
        vmem = pl.BlockSpec(memory_space=pltpu.VMEM)
        F = n_fsdp
        pieces = 2
        ig, grads, norm, factor = pl.pallas_call(
            functools.partial(kernel, n_fsdp, n_rep),
            out_shape=(
                jax.ShapeDtypeStruct((seq, width), BF16),
                jax.ShapeDtypeStruct((wr, chunks * cw), BF16),
                jax.ShapeDtypeStruct((1, 1), F32),
                jax.ShapeDtypeStruct((1, 1), F32),
            ),
            in_specs=[anywhere] * 6 + [scalar] * 2 + [vmem],
            out_specs=(anywhere, anywhere, scalar, scalar),
            scratch_shapes=[
                pltpu.VMEM((seq, width), BF16),
                pltpu.VMEM((seq, width), BF16),
                pltpu.VMEM((seq, qw), BF16),
                pltpu.VMEM(row_lse.shape[::-1], F32),
                pltpu.VMEM((F, 2, half, cols), BF16),
                pltpu.VMEM((F, 2, half, qw), BF16),
                pltpu.VMEM((F, 2, half, seq), BF16),
                pltpu.VMEM((F, 2, half, seq), BF16),
                pltpu.VMEM((seq, cols), F32),
                pltpu.VMEM((seq, qw), F32),
                pltpu.VMEM((seq, cols), BF16),
                pltpu.VMEM((seq, width), BF16),
                pltpu.VMEM((chunks, 2, F, half, cw), BF16),
                pltpu.VMEM((chunks, F, half, cw), BF16),
                pltpu.VMEM((chunks, F, half, cw), BF16),
                pltpu.VMEM((chunks, n_across, half, cw), BF16),
                pltpu.VMEM((chunks, n_across + 1, half, cw), BF16),
                pltpu.VMEM((chunks, 2, half, cw), BF16),
                pltpu.VMEM((2 * F, 8, 128), F32),
                pltpu.VMEM((2, seq, HEAD), F32),
                dma((6,)),
                dma((1 + 2 * chunks,)),
            ]
            + [dma((F,))] * 8
            + [dma((chunks,))] * 2
            + [dma((chunks, pieces, F))] * 2
            + [dma((chunks, pieces, n_across + 2))] * 2
            + [dma((chunks, pieces))] * 2
            + [dma((2 * F,))] * 2,
            compiler_params=pltpu.CompilerParams(
                collective_id=0, has_side_effects=True, vmem_limit_bytes=56 * 2**20
            ),
        )(
            hidden_in, out_grad, attn_saved, row_lse.T,
            w_qkv.reshape(2, half, cols), w_out_t.reshape(2, half, qw),
            doc_lengths, seq_start, freq,
        )
        return ig, grads.astype(F32) * factor[0, 0], norm[0, 0]

    rows = P(("fsdp", "rep"), None)
    in_specs = (rows, rows, rows, rows, P("fsdp", None), P("fsdp", None), rows, P(("fsdp", "rep")))
    return jax.shard_map(
        body, mesh=mesh, in_specs=in_specs, out_specs=(rows, P("fsdp", None), P()), check_vma=False
    )
```
